256 devices in a mesh: rows: 4 (over z_hi, y_lo), cols: 4 (over z_lo), slabs: 4 (over y_hi, x_lo), trial: 4 (over x_hi, core).
Axes of the slice: x: 4 (x_hi: 2, x_lo: 2; x = x_hi * 2 + x_lo), y: 4 (y_hi: 2, y_lo: 2; y = y_hi * 2 + y_lo), z: 8 (z_hi: 2, z_lo: 4; z = z_hi * 4 + z_lo), core: 2. Of those that a mesh axis runs over, the one named last changes fastest.
Arguments:
- field_values: float32 [256, 16, 512, 128], P(('trial', 'rows'), 'cols', 'slabs'), parts along dimension 0, may hold values from 0.5 to 2
- conductance: float32 [256, 16, 512, 128], P(('trial', 'rows'), 'cols', 'slabs'), parts along dimension 0, may hold values from 0.03 to 0.15
- source: float32 [256, 16, 512, 128], P(('trial', 'rows'), 'cols', 'slabs'), parts along dimension 0, may hold values from -0.2 to 0.2
Outputs:
- anomaly: float32 [256, 16, 512, 128], P(('trial', 'rows'), 'cols', 'slabs'), parts along dimension 0
- field_values_end: float32 [256, 16, 512, 128], P(('trial', 'rows'), 'cols', 'slabs'), parts along dimension 0
The draws below stay inside these ranges and needn't reach their ends.
There are 4 independent parts, one for each index of `trial`. The reference program is written for one: setup_inputs(seed, part) draws one part's arguments, and reference() takes and returns one part's arrays. A program takes and returns all parts, laid end to end along the dimension named above; each array names one. Nothing has to cross between parts.
All inputs are finite; a program needn't handle non-finite values.
Results may differ from the reference program's by a relative error of at most 0.00002.
Values sent between devices are 32-bit elements; how exact they have to be, the bound alone decides.
A program may use at most 128 MiB of HBM per device.

```python
import jax
import jax.numpy as jnp
from jax import lax

GRID_J = 64
GRID_I = 16
GRID_K = 512
LEVELS = 128
STEPS = 4


def steps_of(own_key, extent, split, least, largest):
    factor_of, own = 1.0, jax.random.fold_in(own_key, 6)
    for dim, shards_of in split:
        draws = jnp.exp(jax.random.uniform(jax.random.fold_in(own, dim), (shards_of,), jnp.float32, least / len(split), largest / len(split)))
        factor_of = factor_of * jnp.repeat(draws, extent[dim] // shards_of).reshape([-1 if axis == dim else 1 for axis in range(len(extent))])
    return factor_of


def setup_inputs(seed: int = 0, part: int = 0) -> dict:
    keys = jax.random.split(jax.random.key(seed), 4)
    part_splits = jax.random.split(jax.random.fold_in(keys[3], part), 4)
    field_values = jnp.clip(0.5 + 1.5 * jax.random.uniform(part_splits[0], (GRID_J, GRID_I, GRID_K, LEVELS), jnp.float32) ** steps_of(part_splits[0], (GRID_J, GRID_I, GRID_K, LEVELS), ((0, 4), (1, 4), (2, 4)), -0.2, 0.2), 0.5, 2.0)
    conductance = jnp.clip(0.03 + 0.120000007 * jax.random.uniform(part_splits[1], (GRID_J, GRID_I, GRID_K, LEVELS), jnp.float32) ** steps_of(part_splits[1], (GRID_J, GRID_I, GRID_K, LEVELS), ((0, 4), (1, 4), (2, 4)), -0.2, 0.2), 0.03, 0.15)
    source = jnp.clip(jax.random.uniform(part_splits[2], (GRID_J, GRID_I, GRID_K, LEVELS), jnp.float32, -0.2, 0.2) * steps_of(part_splits[2], (GRID_J, GRID_I, GRID_K, LEVELS), ((0, 4), (1, 4), (2, 4)), -0.4, 0.0), -0.2, 0.2)
    return dict(field_values=field_values, conductance=conductance, source=source)


def strip_edges(values, dims):
    for dim in dims:
        values = lax.slice_in_dim(values, 1, values.shape[dim] - 1, axis=dim)
    return values

def neighbour(values, dim, start, dims):
    others = [other for other in dims if other != dim]
    values = strip_edges(values, others)
    return lax.slice_in_dim(values, start, start + values.shape[dim] - 2, axis=dim)

def one_step(padded, conductance, source):
    middle = strip_edges(padded, (0, 1, 2))
    lower = [neighbour(padded, dim, 0, (0, 1, 2)) for dim in (0, 1, 2)]
    upper = [neighbour(padded, dim, 2, (0, 1, 2)) for dim in (0, 1, 2)]
    spread = lower[0] + upper[0] + lower[1] + upper[1] + lower[2] + upper[2] - 6.0 * middle
    return middle + conductance * spread + source

def reference(field_values, conductance, source):
    for step in range(STEPS):
        field_values = one_step(jnp.pad(field_values, ((1, 1), (1, 1), (1, 1), (0, 0)), mode='constant'), conductance, source)
    line_mean = lax.optimization_barrier(jnp.mean(field_values, axis=0, keepdims=True))
    centred = field_values - line_mean
    line_variance = lax.optimization_barrier(jnp.mean(centred * centred, axis=0, keepdims=True))
    anomaly = centred * lax.rsqrt(line_variance + 0.0001)
    return (anomaly, field_values)
```

```python
import functools

import jax
import jax.numpy as jnp
from jax import lax
from jax.experimental import pallas as pl
from jax.experimental.pallas import tpu as pltpu
from jax.sharding import PartitionSpec as P

STEPS = 4
MESH = pl.DeviceIdType.MESH
PAD = 8


def copy_to(src, dst, send, recv, device):
    return pltpu.make_async_remote_copy(
        src_ref=src, dst_ref=dst, send_sem=send, recv_sem=recv, device_id=device, device_id_type=MESH
    )


def kernel(
    sizes, field, conductance, source, anomaly, field_end,
    u, cond, src, last, edge_out, edge_in, part, got1, pair, got2, stats,
    load_sem, col_send, col_recv, row_send, row_recv, slab_send, slab_recv, sum_send, sum_recv, store_sem,
):
    n_rows, n_cols, n_slabs = sizes
    nj, ni, nk, _ = field.shape
    chunks = nk // 8
    r, c, s = lax.axis_index("rows"), lax.axis_index("cols"), lax.axis_index("slabs")
    y_partner = r + 1 - 2 * lax.rem(r, 2)
    z_partner = lax.rem(r + 2, 4)
    half = lax.rem(r, 2) * (ni // 2)
    other = (ni // 2) - half

    def chunk_of(m):
        return jnp.where(lax.rem(m, 2) == 0, m // 2, chunks - 1 - m // 2)

    def at(m):
        return pl.ds(pl.multiple_of(chunk_of(m) * 8, 8), 8)

    def padded(m):
        return pl.ds(pl.multiple_of(chunk_of(m) * 8 + PAD, 8), 8)

    def load(which, m):
        here = (slice(None), slice(None), at(m))
        inside = (0, pl.ds(1, nj), pl.ds(1, ni), padded(m))
        pairs = ((field, u, inside), (conductance, cond, here), (source, src, here))
        start, end, place = pairs[which]
        return pltpu.make_async_copy(start.at[here], end.at[place], load_sem.at[which, m])

    def col_copy(way, n, m):
        a, b = ((1, ni + 1), (ni, 0))[way]
        return copy_to(
            u.at[n, pl.ds(1, nj), a, padded(m)], u.at[n, pl.ds(1, nj), b, padded(m)],
            col_send.at[way, n], col_recv.at[way, n, m], {"cols": c + (-1, 1)[way]},
        )

    def row_copy(way, n, m):
        a, b = ((1, nj + 1), (nj, 0))[way]
        return copy_to(
            u.at[n, a, pl.ds(1, ni), padded(m)], u.at[n, b, pl.ds(1, ni), padded(m)],
            row_send.at[way, n], row_recv.at[way, n, m], {"rows": r + (-1, 1)[way]},
        )

    def slab_copy(way, n):
        return copy_to(
            edge_out.at[way, n], edge_in.at[way, n],
            slab_send.at[way, n], slab_recv.at[way, n], {"slabs": s + (-1, 1)[way]},
        )

    has_col = (c > 0, c < n_cols - 1)
    has_row = (r > 0, r < n_rows - 1)
    has_slab = (s > 0, s < n_slabs - 1)

    def send_faces(n, m):
        for way in range(2):
            pl.when(has_col[way])(lambda way=way: col_copy(way, n, m).start())
        for way in range(2):
            pl.when(has_row[way])(lambda way=way: row_copy(way, n, m).start())
        for way in range(2):
            @pl.when(jnp.logical_and(has_slab[way], m == way))
            def _(way=way):
                k = (PAD, PAD + nk - 1)[way]
                for j in range(nj):
                    for i in range(ni):
                        edge_out[way, n, pl.ds(j * ni + i, 1), :] = u[n, j + 1, i + 1, pl.ds(k, 1), :]
                slab_copy(way, n).start()

    def take_faces(n, m):
        for way in range(2):
            pl.when(has_col[1 - way])(lambda way=way: col_copy(way, n, m).wait_recv())
            pl.when(has_row[1 - way])(lambda way=way: row_copy(way, n, m).wait_recv())
        for way in range(2):
            @pl.when(jnp.logical_and(has_slab[1 - way], m == 1 - way))
            def _(way=way):
                slab_copy(way, n).wait_recv()
                k = (PAD + nk, PAD - 1)[way]
                for j in range(nj):
                    for i in range(ni):
                        u[n, j + 1, i + 1, pl.ds(k, 1), :] = edge_in[way, n, pl.ds(j * ni + i, 1), :]

    def sum_copy(stage, m):
        if stage == 0:
            return copy_to(part.at[m, pl.ds(other, ni // 2)], got1.at[m], sum_send.at[0], sum_recv.at[0, m], {"rows": y_partner})
        if stage == 1:
            return copy_to(pair.at[m], got2.at[m], sum_send.at[1], sum_recv.at[1, m], {"rows": z_partner})
        mine = pl.ds(half, ni // 2)
        return copy_to(stats.at[m, mine], stats.at[m, mine], sum_send.at[2], sum_recv.at[2, m], {"rows": y_partner})

    def stats_arrive(m):
        theirs = pl.ds(other, ni // 2)
        return copy_to(stats.at[m, theirs], stats.at[m, theirs], sum_send.at[2], sum_recv.at[2, m], {"rows": y_partner})

    def store(which, m):
        here = (slice(None), slice(None), at(m))
        start, end = ((last, field_end), (cond, anomaly))[which]
        return pltpu.make_async_copy(start.at[here], end.at[here], store_sem.at[which, m])

    def updated(n, j, i, m, below):
        k0 = chunk_of(m) * 8 + PAD
        middle = u[n, j + 1, i + 1, padded(m), :]
        above = u[n, j + 2, i + 1, padded(m), :]
        spread = below + above + u[n, j + 1, i, padded(m), :] + u[n, j + 1, i + 2, padded(m), :]
        spread = spread + u[n, j + 1, i + 1, pl.ds(k0 - 1, 8), :] + u[n, j + 1, i + 1, pl.ds(k0 + 1, 8), :]
        spread = spread - 6.0 * middle
        return middle, middle + cond[j, i, at(m), :] * spread + src[j, i, at(m), :]

    def step_chunk(n, m):
        def row(j, below):
            out = []
            for i in range(ni):
                middle, new = updated(n, j, i, m, below[i])
                u[n + 1, j + 1, i + 1, padded(m), :] = new
                out.append(middle)
            return tuple(out)

        lax.fori_loop(0, nj, row, tuple(u[n, 0, i + 1, padded(m), :] for i in range(ni)), unroll=2)

    def last_chunk(m):
        n = STEPS - 1

        def row(j, carry):
            below, total = carry
            out, sums = [], []
            for i in range(ni):
                middle, new = updated(n, j, i, m, below[i])
                last[j, i, at(m), :] = new
                out.append(middle)
                sums.append(total[i] + new)
            return tuple(out), tuple(sums)

        zero = jnp.zeros((8, 128), jnp.float32)
        start = tuple(u[n, 0, i + 1, padded(m), :] for i in range(ni))
        _, total = lax.fori_loop(0, nj, row, (start, (zero,) * ni), unroll=2)

        def spread_row(j, squares):
            out = []
            for i in range(ni):
                d = last[j, i, at(m), :] - total[i] * (1.0 / nj)
                out.append(squares[i] + d * d)
            return tuple(out)

        squares = lax.fori_loop(0, nj, spread_row, (zero,) * ni, unroll=4)
        for i in range(ni):
            part[m, i, 0] = total[i]
            part[m, i, 1] = squares[i]

    def joined(a_sum, a_sq, b_sum, b_sq, count):
        d = a_sum - b_sum
        return a_sum + b_sum, a_sq + b_sq + d * d * (0.5 / count)

    for m in range(chunks):
        load(0, m).start()
    for m in range(chunks):
        load(1, m).start()
        load(2, m).start()
    barrier = pltpu.get_barrier_semaphore()
    for way in range(2):
        step = (-1, 1)[way]
        pl.when(has_col[way])(lambda step=step: pl.semaphore_signal(barrier, inc=1, device_id={"cols": c + step}, device_id_type=MESH))
        pl.when(has_slab[way])(lambda step=step: pl.semaphore_signal(barrier, inc=1, device_id={"slabs": s + step}, device_id_type=MESH))
    for d in range(1, n_rows):
        pl.semaphore_signal(barrier, inc=1, device_id={"rows": lax.rem(r + d, n_rows)}, device_id_type=MESH)

    zero = jnp.zeros((8, 128), jnp.float32)

    def clear_cols(i):
        def body(q, x):
            n, j = q // nj, lax.rem(q, nj)
            for k in range(chunks):
                u[n, j + 1, i, pl.ds(PAD + 8 * k, 8), :] = zero
            return x
        lax.fori_loop(0, STEPS * nj, body, 0)

    def clear_rows(j):
        def body(q, x):
            n, i = q // ni, lax.rem(q, ni)
            for k in range(chunks):
                u[n, j, i + 1, pl.ds(PAD + 8 * k, 8), :] = zero
            return x
        lax.fori_loop(0, STEPS * ni, body, 0)

    def clear_slabs(k):
        def body(q, x):
            n, j = q // nj, lax.rem(q, nj)
            for i in range(ni):
                u[n, j + 1, i + 1, pl.ds(k, 8), :] = zero
            return x
        lax.fori_loop(0, STEPS * nj, body, 0)

    pl.when(c == 0)(lambda: clear_cols(0))
    pl.when(c == n_cols - 1)(lambda: clear_cols(ni + 1))
    pl.when(r == 0)(lambda: clear_rows(0))
    pl.when(r == n_rows - 1)(lambda: clear_rows(nj + 1))
    pl.when(s == 0)(lambda: clear_slabs(0))
    pl.when(s == n_slabs - 1)(lambda: clear_slabs(PAD + nk))

    one = lambda flag: jnp.where(flag, 1, 0)
    pl.semaphore_wait(barrier, n_rows - 1 + one(has_col[0]) + one(has_col[1]) + one(has_slab[0]) + one(has_slab[1]))

    def first(m, x):
        load(0, m).wait()
        send_faces(0, m)
        return x

    lax.fori_loop(0, chunks, first, 0)

    def steps(q, x):
        n, m = q // chunks, lax.rem(q, chunks)

        @pl.when(n == 0)
        def _():
            load(1, m).wait()
            load(2, m).wait()

        take_faces(n, m)
        step_chunk(n, m)
        send_faces(n + 1, m)
        return x

    lax.fori_loop(0, (STEPS - 1) * chunks, steps, 0)

    def stage1(m):
        take_faces(STEPS - 1, m)
        last_chunk(m)
        store(0, m).start()
        sum_copy(0, m).start()

    def stage2(m):
        sum_copy(0, m).wait_recv()
        for i in range(ni // 2):
            total, squares = joined(part[m, half + i, 0], part[m, half + i, 1], got1[m, i, 0], got1[m, i, 1], nj)
            pair[m, i, 0] = total
            pair[m, i, 1] = squares
        sum_copy(1, m).start()

    def stage3(m):
        sum_copy(1, m).wait_recv()
        count = nj * n_rows
        for i in range(ni // 2):
            total, squares = joined(pair[m, i, 0], pair[m, i, 1], got2[m, i, 0], got2[m, i, 1], 2 * nj)
            stats[m, half + i, 0] = total * (1.0 / count)
            stats[m, half + i, 1] = lax.rsqrt(squares * (1.0 / count) + 0.0001)
        sum_copy(2, m).start()

    def stage4(m):
        stats_arrive(m).wait_recv()
        mean = [stats[m, i, 0] for i in range(ni)]
        scale = [stats[m, i, 1] for i in range(ni)]

        def row(j, x):
            for i in range(ni):
                cond[j, i, at(m), :] = (last[j, i, at(m), :] - mean[i]) * scale[i]
            return x

        lax.fori_loop(0, nj, row, 0, unroll=4)
        store(1, m).start()

    lags = (0, 2, 5, 7)

    def tail(t, x):
        for lag, stage in zip(lags, (stage1, stage2, stage3, stage4)):
            m = t - lag
            pl.when(jnp.logical_and(m >= 0, m < chunks))(lambda m=m, stage=stage: stage(m))
        return x

    lax.fori_loop(0, chunks + lags[-1], tail, 0)

    for way in range(2):
        for n in range(STEPS):
            a = (1, ni)[way]
            whole = u.at[n, pl.ds(1, nj), a, pl.ds(PAD, nk)]
            pl.when(has_col[way])(lambda way=way, n=n, whole=whole: copy_to(whole, whole, col_send.at[way, n], col_recv.at[way, n, 0], {"cols": c + (-1, 1)[way]}).wait_send())
            b = (1, nj)[way]
            face = u.at[n, b, pl.ds(1, ni), pl.ds(PAD, nk)]
            pl.when(has_row[way])(lambda way=way, n=n, face=face: copy_to(face, face, row_send.at[way, n], row_recv.at[way, n, 0], {"rows": r + (-1, 1)[way]}).wait_send())
            pl.when(has_slab[way])(lambda way=way, n=n: slab_copy(way, n).wait_send())
    for stage, ref in enumerate((got1, pair, got1)):
        copy_to(ref, ref, sum_send.at[stage], sum_recv.at[stage, 0], {"rows": y_partner}).wait_send()

    def stored(m, x):
        store(0, m).wait()
        store(1, m).wait()
        return x

    lax.fori_loop(0, chunks, stored, 0)


def solution(mesh):
    sizes = (mesh.shape["rows"], mesh.shape["cols"], mesh.shape["slabs"])

    def on_device(field_values, conductance, source):
        shape = field_values.shape
        nj, ni, nk, levels = shape
        chunks = nk // 8
        f32 = jnp.float32
        sem = pltpu.SemaphoreType.DMA
        return pl.pallas_call(
            functools.partial(kernel, sizes),
            out_shape=(jax.ShapeDtypeStruct(shape, f32), jax.ShapeDtypeStruct(shape, f32)),
            in_specs=[pl.BlockSpec(memory_space=pltpu.HBM)] * 3,
            out_specs=(pl.BlockSpec(memory_space=pltpu.HBM),) * 2,
            scratch_shapes=[
                pltpu.VMEM((STEPS, nj + 2, ni + 2, nk + 2 * PAD, levels), f32),
                pltpu.VMEM(shape, f32),
                pltpu.VMEM(shape, f32),
                pltpu.VMEM(shape, f32),
                pltpu.VMEM((2, STEPS, nj * ni, levels), f32),
                pltpu.VMEM((2, STEPS, nj * ni, levels), f32),
                pltpu.VMEM((chunks, ni, 2, 8, levels), f32),
                pltpu.VMEM((chunks, ni // 2, 2, 8, levels), f32),
                pltpu.VMEM((chunks, ni // 2, 2, 8, levels), f32),
                pltpu.VMEM((chunks, ni // 2, 2, 8, levels), f32),
                pltpu.VMEM((chunks, ni, 2, 8, levels), f32),
                sem((3, chunks)),
                sem((2, STEPS)),
                sem((2, STEPS, chunks)),
                sem((2, STEPS)),
                sem((2, STEPS, chunks)),
                sem((2, STEPS)),
                sem((2, STEPS)),
                sem((3,)),
                sem((3, chunks)),
                sem((2, chunks)),
            ],
            compiler_params=pltpu.CompilerParams(
                collective_id=0, has_side_effects=True, vmem_limit_bytes=60 * 2**20
            ),
            name="heat",
        )(field_values, conductance, source)

    spec = P(("trial", "rows"), "cols", "slabs", None)
    return jax.shard_map(on_device, mesh=mesh, in_specs=(spec,) * 3, out_specs=(spec,) * 2, check_vma=False)
```

```python
import functools

import jax
import jax.numpy as jnp
from jax import lax
from jax.experimental import pallas as pl
from jax.experimental.pallas import tpu as pltpu
from jax.sharding import PartitionSpec as P

STEPS = 4
MESH = pl.DeviceIdType.MESH
LATE = 2
PAD = 8


def copy_to(src, dst, send, recv, device):
    return pltpu.make_async_remote_copy(
        src_ref=src, dst_ref=dst, send_sem=send, recv_sem=recv, device_id=device, device_id_type=MESH
    )


def kernel(
    sizes, field, conductance, source, anomaly, field_end,
    u, cond, src, last, edge_out, edge_in, relay, part, got1, pair, got2, stats,
    relay_send, relay_recv, load_sem, col_send, col_recv, row_send, row_recv, slab_send, slab_recv, sum_send, sum_recv, store_sem,
):
    n_rows, n_cols, n_slabs = sizes
    nj, ni, nk, _ = field.shape
    chunks = nk // 8
    r, c, s = lax.axis_index("rows"), lax.axis_index("cols"), lax.axis_index("slabs")
    y_partner = r + 1 - 2 * lax.rem(r, 2)
    z_partner = lax.rem(r + 2, 4)
    half = lax.rem(r, 2) * (ni // 2)
    other = (ni // 2) - half

    def chunk_of(m):
        return jnp.where(lax.rem(m, 2) == 0, m // 2, chunks - 1 - m // 2)

    def at(m):
        return pl.ds(pl.multiple_of(chunk_of(m) * 8, 8), 8)

    def padded(m):
        return pl.ds(pl.multiple_of(chunk_of(m) * 8 + PAD, 8), 8)

    def load(which, m):
        here = (slice(None), slice(None), at(m))
        inside = (0, pl.ds(1, nj), pl.ds(1, ni), padded(m))
        pairs = ((field, u, inside), (conductance, cond, here), (source, src, here))
        start, end, place = pairs[which]
        return pltpu.make_async_copy(start.at[here], end.at[place], load_sem.at[which, m])

    def col_copy(way, n, m):
        a, b = ((1, ni + 1), (ni, 0))[way]
        return copy_to(
            u.at[n, pl.ds(1, nj), a, padded(m)], u.at[n, pl.ds(1, nj), b, padded(m)],
            col_send.at[way, n], col_recv.at[way, n, m], {"cols": c + (-1, 1)[way]},
        )

    def row_copy(way, n, m):
        a, b = ((1, nj + 1), (nj, 0))[way]
        return copy_to(
            u.at[n, a, pl.ds(1, ni), padded(m)], u.at[n, b, pl.ds(1, ni), padded(m)],
            row_send.at[way, n], row_recv.at[way, n, m], {"rows": r + (-1, 1)[way]},
        )

    def detour_copy(way, n, m):
        return copy_to(
            u.at[n, (1, nj)[way], pl.ds(1, ni), padded(m)], relay.at[n, m // 2],
            row_send.at[way, n], relay_recv.at[n, m // 2], {"rows": r + (1, -1)[way]},
        )

    def forward_copy(way, n, m):
        return copy_to(
            relay.at[n, m // 2], u.at[n, (nj + 1, 0)[way], pl.ds(1, ni), padded(m)],
            relay_send.at[n], row_recv.at[way, n, m], {"rows": r + (-2, 2)[way]},
        )

    crosses = (r == 2, r == 1)
    forwards = (r == 3, r == 0)

    def forward(n, m):
        for way in range(2):
            @pl.when(jnp.logical_and(forwards[way], lax.rem(m, 2) == 1))
            def _(way=way):
                detour_copy(way, n, m).wait_recv()
                forward_copy(way, n, m).start()

    def slab_copy(way, n):
        return copy_to(
            edge_out.at[way, n], edge_in.at[way, n],
            slab_send.at[way, n], slab_recv.at[way, n], {"slabs": s + (-1, 1)[way]},
        )

    has_col = (c > 0, c < n_cols - 1)
    has_row = (r > 0, r < n_rows - 1)
    has_slab = (s > 0, s < n_slabs - 1)

    def send_faces(n, m):
        for way in range(2):
            pl.when(has_col[way])(lambda way=way: col_copy(way, n, m).start())
        for way in range(2):
            detour = jnp.logical_and(crosses[way], lax.rem(m, 2) == 1)
            pl.when(detour)(lambda way=way: detour_copy(way, n, m).start())
            pl.when(jnp.logical_and(has_row[way], jnp.logical_not(detour)))(lambda way=way: row_copy(way, n, m).start())
        for way in range(2):
            @pl.when(jnp.logical_and(has_slab[way], m == way))
            def _(way=way):
                k = (PAD, PAD + nk - 1)[way]
                for j in range(nj):
                    for i in range(ni):
                        edge_out[way, n, pl.ds(j * ni + i, 1), :] = u[n, j + 1, i + 1, pl.ds(k, 1), :]
                slab_copy(way, n).start()

    def take_faces(n, m):
        for way in range(2):
            pl.when(has_col[1 - way])(lambda way=way: col_copy(way, n, m).wait_recv())
            pl.when(has_row[1 - way])(lambda way=way: row_copy(way, n, m).wait_recv())
        for way in range(2):
            @pl.when(jnp.logical_and(has_slab[1 - way], m == 1 - way))
            def _(way=way):
                slab_copy(way, n).wait_recv()
                k = (PAD + nk, PAD - 1)[way]
                for j in range(nj):
                    for i in range(ni):
                        u[n, j + 1, i + 1, pl.ds(k, 1), :] = edge_in[way, n, pl.ds(j * ni + i, 1), :]

    def sum_copy(stage, m):
        if stage == 0:
            return copy_to(part.at[m, pl.ds(other, ni // 2)], got1.at[m], sum_send.at[0], sum_recv.at[0, m], {"rows": y_partner})
        if stage == 1:
            return copy_to(pair.at[m], got2.at[m], sum_send.at[1], sum_recv.at[1, m], {"rows": z_partner})
        mine = pl.ds(half, ni // 2)
        return copy_to(stats.at[m, mine], stats.at[m, mine], sum_send.at[2], sum_recv.at[2, m], {"rows": y_partner})

    def stats_arrive(m):
        theirs = pl.ds(other, ni // 2)
        return copy_to(stats.at[m, theirs], stats.at[m, theirs], sum_send.at[2], sum_recv.at[2, m], {"rows": y_partner})

    def store(which, m):
        here = (slice(None), slice(None), at(m))
        start, end = ((last, field_end), (cond, anomaly))[which]
        return pltpu.make_async_copy(start.at[here], end.at[here], store_sem.at[which, m])

    def updated(n, j, i, m, below):
        k0 = chunk_of(m) * 8 + PAD
        middle = u[n, j + 1, i + 1, padded(m), :]
        above = u[n, j + 2, i + 1, padded(m), :]
        spread = below + above + u[n, j + 1, i, padded(m), :] + u[n, j + 1, i + 2, padded(m), :]
        spread = spread + u[n, j + 1, i + 1, pl.ds(k0 - 1, 8), :] + u[n, j + 1, i + 1, pl.ds(k0 + 1, 8), :]
        spread = spread - 6.0 * middle
        return middle, middle + cond[j, i, at(m), :] * spread + src[j, i, at(m), :]

    def step_chunk(n, m):
        def row(j, below):
            out = []
            for i in range(ni):
                middle, new = updated(n, j, i, m, below[i])
                u[n + 1, j + 1, i + 1, padded(m), :] = new
                out.append(middle)
            return tuple(out)

        lax.fori_loop(0, nj, row, tuple(u[n, 0, i + 1, padded(m), :] for i in range(ni)), unroll=2)

    def last_chunk(m):
        n = STEPS - 1

        def row(j, carry):
            below, total = carry
            out, sums = [], []
            for i in range(ni):
                middle, new = updated(n, j, i, m, below[i])
                last[j, i, at(m), :] = new
                out.append(middle)
                sums.append(total[i] + new)
            return tuple(out), tuple(sums)

        zero = jnp.zeros((8, 128), jnp.float32)
        start = tuple(u[n, 0, i + 1, padded(m), :] for i in range(ni))
        _, total = lax.fori_loop(0, nj, row, (start, (zero,) * ni), unroll=2)

        def spread_row(j, squares):
            out = []
            for i in range(ni):
                d = last[j, i, at(m), :] - total[i] * (1.0 / nj)
                out.append(squares[i] + d * d)
            return tuple(out)

        squares = lax.fori_loop(0, nj, spread_row, (zero,) * ni, unroll=4)
        for i in range(ni):
            part[m, i, 0] = total[i]
            part[m, i, 1] = squares[i]

    def joined(a_sum, a_sq, b_sum, b_sq, count):
        d = a_sum - b_sum
        return a_sum + b_sum, a_sq + b_sq + d * d * (0.5 / count)

    for m in range(chunks):
        load(0, m).start()
    for m in range(chunks):
        load(1, m).start()
        load(2, m).start()
    barrier = pltpu.get_barrier_semaphore()
    for way in range(2):
        step = (-1, 1)[way]
        pl.when(has_col[way])(lambda step=step: pl.semaphore_signal(barrier, inc=1, device_id={"cols": c + step}, device_id_type=MESH))
        pl.when(has_slab[way])(lambda step=step: pl.semaphore_signal(barrier, inc=1, device_id={"slabs": s + step}, device_id_type=MESH))
    for d in range(1, n_rows):
        pl.semaphore_signal(barrier, inc=1, device_id={"rows": lax.rem(r + d, n_rows)}, device_id_type=MESH)

    zero = jnp.zeros((8, 128), jnp.float32)

    def clear_cols(i):
        def body(q, x):
            n, j = q // nj, lax.rem(q, nj)
            for k in range(chunks):
                u[n, j + 1, i, pl.ds(PAD + 8 * k, 8), :] = zero
            return x
        lax.fori_loop(0, STEPS * nj, body, 0)

    def clear_rows(j):
        def body(q, x):
            n, i = q // ni, lax.rem(q, ni)
            for k in range(chunks):
                u[n, j, i + 1, pl.ds(PAD + 8 * k, 8), :] = zero
            return x
        lax.fori_loop(0, STEPS * ni, body, 0)

    def clear_slabs(k):
        def body(q, x):
            n, j = q // nj, lax.rem(q, nj)
            for i in range(ni):
                u[n, j + 1, i + 1, pl.ds(k, 8), :] = zero
            return x
        lax.fori_loop(0, STEPS * nj, body, 0)

    pl.when(c == 0)(lambda: clear_cols(0))
    pl.when(c == n_cols - 1)(lambda: clear_cols(ni + 1))
    pl.when(r == 0)(lambda: clear_rows(0))
    pl.when(r == n_rows - 1)(lambda: clear_rows(nj + 1))
    pl.when(s == 0)(lambda: clear_slabs(0))
    pl.when(s == n_slabs - 1)(lambda: clear_slabs(PAD + nk))

    one = lambda flag: jnp.where(flag, 1, 0)
    pl.semaphore_wait(barrier, n_rows - 1 + one(has_col[0]) + one(has_col[1]) + one(has_slab[0]) + one(has_slab[1]))

    def first(m, x):
        load(0, m).wait()
        send_faces(0, m)
        forward(0, m)
        return x

    lax.fori_loop(0, chunks, first, 0)

    def forward_late(q):
        p = q - LATE
        pl.when(p >= 0)(lambda: forward(p // chunks + 1, lax.rem(p, chunks)))

    def steps(q, x):
        n, m = q // chunks, lax.rem(q, chunks)
        forward_late(q)

        @pl.when(n == 0)
        def _():
            load(1, m).wait()
            load(2, m).wait()

        take_faces(n, m)
        step_chunk(n, m)
        send_faces(n + 1, m)
        return x

    lax.fori_loop(0, (STEPS - 1) * chunks, steps, 0)

    def stage1(m):
        take_faces(STEPS - 1, m)
        last_chunk(m)
        store(0, m).start()
        sum_copy(0, m).start()

    def stage2(m):
        sum_copy(0, m).wait_recv()
        for i in range(ni // 2):
            total, squares = joined(part[m, half + i, 0], part[m, half + i, 1], got1[m, i, 0], got1[m, i, 1], nj)
            pair[m, i, 0] = total
            pair[m, i, 1] = squares
        sum_copy(1, m).start()

    def stage3(m):
        sum_copy(1, m).wait_recv()
        count = nj * n_rows
        for i in range(ni // 2):
            total, squares = joined(pair[m, i, 0], pair[m, i, 1], got2[m, i, 0], got2[m, i, 1], 2 * nj)
            stats[m, half + i, 0] = total * (1.0 / count)
            stats[m, half + i, 1] = lax.rsqrt(squares * (1.0 / count) + 0.0001)
        sum_copy(2, m).start()

    def stage4(m):
        stats_arrive(m).wait_recv()
        mean = [stats[m, i, 0] for i in range(ni)]
        scale = [stats[m, i, 1] for i in range(ni)]

        def row(j, x):
            for i in range(ni):
                cond[j, i, at(m), :] = (last[j, i, at(m), :] - mean[i]) * scale[i]
            return x

        lax.fori_loop(0, nj, row, 0, unroll=4)
        store(1, m).start()

    lags = (0, 2, 5, 7)

    def tail(t, x):
        pl.when(t < LATE)(lambda: forward_late(t + (STEPS - 1) * chunks))
        for lag, stage in zip(lags, (stage1, stage2, stage3, stage4)):
            m = t - lag
            pl.when(jnp.logical_and(m >= 0, m < chunks))(lambda m=m, stage=stage: stage(m))
        return x

    lax.fori_loop(0, chunks + lags[-1], tail, 0)

    for way in range(2):
        for n in range(STEPS):
            a = (1, ni)[way]
            whole = u.at[n, pl.ds(1, nj), a, pl.ds(PAD, nk)]
            pl.when(has_col[way])(lambda way=way, n=n, whole=whole: copy_to(whole, whole, col_send.at[way, n], col_recv.at[way, n, 0], {"cols": c + (-1, 1)[way]}).wait_send())
            b = (1, nj)[way]
            face = u.at[n, b, pl.ds(1, ni), pl.ds(PAD, nk)]
            pl.when(has_row[way])(lambda way=way, n=n, face=face: copy_to(face, face, row_send.at[way, n], row_recv.at[way, n, 0], {"rows": r + (-1, 1)[way]}).wait_send())
            pl.when(has_slab[way])(lambda way=way, n=n: slab_copy(way, n).wait_send())
    for n in range(STEPS):
        for way in range(2):
            @pl.when(forwards[way])
            def _(n=n, way=way):
                copy_to(relay.at[n], relay.at[n], relay_send.at[n], relay_recv.at[n, 0], {"rows": r + (-2, 2)[way]}).wait_send()
    for stage, ref in enumerate((got1, pair, got1)):
        copy_to(ref, ref, sum_send.at[stage], sum_recv.at[stage, 0], {"rows": y_partner}).wait_send()

    def stored(m, x):
        store(0, m).wait()
        store(1, m).wait()
        return x

    lax.fori_loop(0, chunks, stored, 0)


def solution(mesh):
    sizes = (mesh.shape["rows"], mesh.shape["cols"], mesh.shape["slabs"])

    def on_device(field_values, conductance, source):
        shape = field_values.shape
        nj, ni, nk, levels = shape
        chunks = nk // 8
        f32 = jnp.float32
        sem = pltpu.SemaphoreType.DMA
        return pl.pallas_call(
            functools.partial(kernel, sizes),
            out_shape=(jax.ShapeDtypeStruct(shape, f32), jax.ShapeDtypeStruct(shape, f32)),
            in_specs=[pl.BlockSpec(memory_space=pltpu.HBM)] * 3,
            out_specs=(pl.BlockSpec(memory_space=pltpu.HBM),) * 2,
            scratch_shapes=[
                pltpu.VMEM((STEPS, nj + 2, ni + 2, nk + 2 * PAD, levels), f32),
                pltpu.VMEM(shape, f32),
                pltpu.VMEM(shape, f32),
                pltpu.VMEM(shape, f32),
                pltpu.VMEM((2, STEPS, nj * ni, levels), f32),
                pltpu.VMEM((2, STEPS, nj * ni, levels), f32),
                pltpu.VMEM((STEPS, chunks // 2, ni, 8, levels), f32),
                pltpu.VMEM((chunks, ni, 2, 8, levels), f32),
                pltpu.VMEM((chunks, ni // 2, 2, 8, levels), f32),
                pltpu.VMEM((chunks, ni // 2, 2, 8, levels), f32),
                pltpu.VMEM((chunks, ni // 2, 2, 8, levels), f32),
                pltpu.VMEM((chunks, ni, 2, 8, levels), f32),
                sem((STEPS,)),
                sem((STEPS, chunks // 2)),
                sem((3, chunks)),
                sem((2, STEPS)),
                sem((2, STEPS, chunks)),
                sem((2, STEPS)),
                sem((2, STEPS, chunks)),
                sem((2, STEPS)),
                sem((2, STEPS)),
                sem((3,)),
                sem((3, chunks)),
                sem((2, chunks)),
            ],
            compiler_params=pltpu.CompilerParams(
                collective_id=0, has_side_effects=True, vmem_limit_bytes=60 * 2**20
            ),
            name="heat",
        )(field_values, conductance, source)

    spec = P(("trial", "rows"), "cols", "slabs", None)
    return jax.shard_map(on_device, mesh=mesh, in_specs=(spec,) * 3, out_specs=(spec,) * 2, check_vma=False)
```

```python
import functools

import jax
import jax.numpy as jnp
from jax import lax
from jax.experimental import pallas as pl
from jax.experimental.pallas import tpu as pltpu
from jax.sharding import PartitionSpec as P

STEPS = 4
MESH = pl.DeviceIdType.MESH
LATE = 3
PAD = 8


def copy_to(src, dst, send, recv, device):
    return pltpu.make_async_remote_copy(
        src_ref=src, dst_ref=dst, send_sem=send, recv_sem=recv, device_id=device, device_id_type=MESH
    )


def kernel(
    sizes, field, conductance, source, last, stats,
    u, cond, src, edge_out, edge_in, relay, part, got1, pair, got2,
    relay_send, relay_recv, load_sem, col_send, col_recv, row_send, row_recv, slab_send, slab_recv, sum_send, sum_recv,
):
    n_rows, n_cols, n_slabs = sizes
    nj, ni, nk, _ = field.shape
    chunks = nk // 8
    r, c, s = lax.axis_index("rows"), lax.axis_index("cols"), lax.axis_index("slabs")
    y_partner = r + 1 - 2 * lax.rem(r, 2)
    z_partner = lax.rem(r + 2, 4)
    half = lax.rem(r, 2) * (ni // 2)
    other = (ni // 2) - half

    def chunk_of(m):
        return jnp.where(lax.rem(m, 2) == 0, m // 2, chunks - 1 - m // 2)

    def at(m):
        return pl.ds(pl.multiple_of(chunk_of(m) * 8, 8), 8)

    def padded(m):
        return pl.ds(pl.multiple_of(chunk_of(m) * 8 + PAD, 8), 8)

    def load(which, m):
        here = (slice(None), slice(None), at(m))
        inside = (0, pl.ds(1, nj), pl.ds(1, ni), padded(m))
        pairs = ((field, u, inside), (conductance, cond, here), (source, src, here))
        start, end, place = pairs[which]
        return pltpu.make_async_copy(start.at[here], end.at[place], load_sem.at[which, m])

    def col_copy(way, n, m):
        a, b = ((1, ni + 1), (ni, 0))[way]
        return copy_to(
            u.at[n, pl.ds(1, nj), a, padded(m)], u.at[n, pl.ds(1, nj), b, padded(m)],
            col_send.at[way, n], col_recv.at[way, n, m], {"cols": c + (-1, 1)[way]},
        )

    def row_copy(way, n, m):
        a, b = ((1, nj + 1), (nj, 0))[way]
        return copy_to(
            u.at[n, a, pl.ds(1, ni), padded(m)], u.at[n, b, pl.ds(1, ni), padded(m)],
            row_send.at[way, n], row_recv.at[way, n, m], {"rows": r + (-1, 1)[way]},
        )

    def detour_copy(way, n, m):
        return copy_to(
            u.at[n, (1, nj)[way], pl.ds(1, ni), padded(m)], relay.at[n, m // 2],
            row_send.at[way, n], relay_recv.at[n, m // 2], {"rows": r + (1, -1)[way]},
        )

    def forward_copy(way, n, m):
        return copy_to(
            relay.at[n, m // 2], u.at[n, (nj + 1, 0)[way], pl.ds(1, ni), padded(m)],
            relay_send.at[n], row_recv.at[way, n, m], {"rows": r + (-2, 2)[way]},
        )

    crosses = (r == 2, r == 1)
    forwards = (r == 3, r == 0)

    def forward(n, m):
        for way in range(2):
            @pl.when(jnp.logical_and(forwards[way], lax.rem(m, 2) == 1))
            def _(way=way):
                detour_copy(way, n, m).wait_recv()
                forward_copy(way, n, m).start()

    def slab_copy(way, n):
        return copy_to(
            edge_out.at[way, n], edge_in.at[way, n],
            slab_send.at[way, n], slab_recv.at[way, n], {"slabs": s + (-1, 1)[way]},
        )

    has_col = (c > 0, c < n_cols - 1)
    has_row = (r > 0, r < n_rows - 1)
    has_slab = (s > 0, s < n_slabs - 1)

    def send_faces(n, m):
        for way in range(2):
            pl.when(has_col[way])(lambda way=way: col_copy(way, n, m).start())
        for way in range(2):
            detour = jnp.logical_and(crosses[way], lax.rem(m, 2) == 1)
            pl.when(detour)(lambda way=way: detour_copy(way, n, m).start())
            pl.when(jnp.logical_and(has_row[way], jnp.logical_not(detour)))(lambda way=way: row_copy(way, n, m).start())
        for way in range(2):
            @pl.when(jnp.logical_and(has_slab[way], m == way))
            def _(way=way):
                k = (PAD, PAD + nk - 1)[way]
                for j in range(nj):
                    for i in range(ni):
                        edge_out[way, n, pl.ds(j * ni + i, 1), :] = u[n, j + 1, i + 1, pl.ds(k, 1), :]
                slab_copy(way, n).start()

    def take_faces(n, m):
        for way in range(2):
            pl.when(has_col[1 - way])(lambda way=way: col_copy(way, n, m).wait_recv())
            pl.when(has_row[1 - way])(lambda way=way: row_copy(way, n, m).wait_recv())
        for way in range(2):
            @pl.when(jnp.logical_and(has_slab[1 - way], m == 1 - way))
            def _(way=way):
                slab_copy(way, n).wait_recv()
                k = (PAD + nk, PAD - 1)[way]
                for j in range(nj):
                    for i in range(ni):
                        u[n, j + 1, i + 1, pl.ds(k, 1), :] = edge_in[way, n, pl.ds(j * ni + i, 1), :]

    def sum_copy(stage, m):
        if stage == 0:
            return copy_to(part.at[m, pl.ds(other, ni // 2)], got1.at[m], sum_send.at[0], sum_recv.at[0, m], {"rows": y_partner})
        if stage == 1:
            return copy_to(pair.at[m], got2.at[m], sum_send.at[1], sum_recv.at[1, m], {"rows": z_partner})
        mine = stats.at[:, pl.ds(half, ni // 2), at(m)]
        return copy_to(mine, mine, sum_send.at[2], sum_recv.at[2, m], {"rows": y_partner})

    def stats_arrive(m):
        theirs = stats.at[:, pl.ds(other, ni // 2), at(m)]
        return copy_to(theirs, theirs, sum_send.at[2], sum_recv.at[2, m], {"rows": y_partner})

    def updated(n, j, i, m, below):
        k0 = chunk_of(m) * 8 + PAD
        middle = u[n, j + 1, i + 1, padded(m), :]
        above = u[n, j + 2, i + 1, padded(m), :]
        spread = below + above + u[n, j + 1, i, padded(m), :] + u[n, j + 1, i + 2, padded(m), :]
        spread = spread + u[n, j + 1, i + 1, pl.ds(k0 - 1, 8), :] + u[n, j + 1, i + 1, pl.ds(k0 + 1, 8), :]
        spread = spread - 6.0 * middle
        return middle, middle + cond[j, i, at(m), :] * spread + src[j, i, at(m), :]

    def step_chunk(n, m):
        def row(j, below):
            out = []
            for i in range(ni):
                middle, new = updated(n, j, i, m, below[i])
                u[n + 1, j + 1, i + 1, padded(m), :] = new
                out.append(middle)
            return tuple(out)

        lax.fori_loop(0, nj, row, tuple(u[n, 0, i + 1, padded(m), :] for i in range(ni)), unroll=2)

    def last_chunk(m):
        n = STEPS - 1

        def row(j, carry):
            below, total = carry
            out, sums = [], []
            for i in range(ni):
                middle, new = updated(n, j, i, m, below[i])
                last[j, i, at(m), :] = new
                out.append(middle)
                sums.append(total[i] + new)
            return tuple(out), tuple(sums)

        zero = jnp.zeros((8, 128), jnp.float32)
        start = tuple(u[n, 0, i + 1, padded(m), :] for i in range(ni))
        _, total = lax.fori_loop(0, nj, row, (start, (zero,) * ni), unroll=2)

        def spread_row(j, squares):
            out = []
            for i in range(ni):
                d = last[j, i, at(m), :] - total[i] * (1.0 / nj)
                out.append(squares[i] + d * d)
            return tuple(out)

        squares = lax.fori_loop(0, nj, spread_row, (zero,) * ni, unroll=4)
        for i in range(ni):
            part[m, i, 0] = total[i]
            part[m, i, 1] = squares[i]

    def joined(a_sum, a_sq, b_sum, b_sq, count):
        d = a_sum - b_sum
        return a_sum + b_sum, a_sq + b_sq + d * d * (0.5 / count)

    barrier = pltpu.get_barrier_semaphore()
    for way in range(2):
        step = (-1, 1)[way]
        pl.when(has_col[way])(lambda step=step: pl.semaphore_signal(barrier, inc=1, device_id={"cols": c + step}, device_id_type=MESH))
        pl.when(has_slab[way])(lambda step=step: pl.semaphore_signal(barrier, inc=1, device_id={"slabs": s + step}, device_id_type=MESH))
    for d in range(1, n_rows):
        pl.semaphore_signal(barrier, inc=1, device_id={"rows": lax.rem(r + d, n_rows)}, device_id_type=MESH)
    for m in range(chunks):
        load(0, m).start()
    for m in range(chunks):
        load(1, m).start()
        load(2, m).start()

    zero = jnp.zeros((8, 128), jnp.float32)

    def clear_cols(i):
        def body(q, x):
            n, j = q // nj, lax.rem(q, nj)
            for k in range(chunks):
                u[n, j + 1, i, pl.ds(PAD + 8 * k, 8), :] = zero
            return x
        lax.fori_loop(0, STEPS * nj, body, 0)

    def clear_rows(j):
        def body(q, x):
            n, i = q // ni, lax.rem(q, ni)
            for k in range(chunks):
                u[n, j, i + 1, pl.ds(PAD + 8 * k, 8), :] = zero
            return x
        lax.fori_loop(0, STEPS * ni, body, 0)

    def clear_slabs(k):
        def body(q, x):
            n, j = q // nj, lax.rem(q, nj)
            for i in range(ni):
                u[n, j + 1, i + 1, pl.ds(k, 8), :] = zero
            return x
        lax.fori_loop(0, STEPS * nj, body, 0)

    pl.when(c == 0)(lambda: clear_cols(0))
    pl.when(c == n_cols - 1)(lambda: clear_cols(ni + 1))
    pl.when(r == 0)(lambda: clear_rows(0))
    pl.when(r == n_rows - 1)(lambda: clear_rows(nj + 1))
    pl.when(s == 0)(lambda: clear_slabs(0))
    pl.when(s == n_slabs - 1)(lambda: clear_slabs(PAD + nk))

    one = lambda flag: jnp.where(flag, 1, 0)
    pl.semaphore_wait(barrier, n_rows - 1 + one(has_col[0]) + one(has_col[1]) + one(has_slab[0]) + one(has_slab[1]))

    def first(m, x):
        load(0, m).wait()
        send_faces(0, m)
        forward(0, m)
        return x

    lax.fori_loop(0, chunks, first, 0)

    def forward_late(q):
        p = q - LATE
        pl.when(p >= 0)(lambda: forward(p // chunks + 1, lax.rem(p, chunks)))

    def steps(q, x):
        n, m = q // chunks, lax.rem(q, chunks)
        forward_late(q)

        @pl.when(n == 0)
        def _():
            load(1, m).wait()
            load(2, m).wait()

        take_faces(n, m)
        step_chunk(n, m)
        pl.when(q > 0)(lambda: send_faces((q - 1) // chunks + 1, lax.rem(q - 1, chunks)))
        return x

    lax.fori_loop(0, (STEPS - 1) * chunks, steps, 0)

    send_faces(STEPS - 1, chunks - 1)

    def stage1(m):
        take_faces(STEPS - 1, m)
        last_chunk(m)
        sum_copy(0, m).start()

    def stage2(m):
        sum_copy(0, m).wait_recv()
        for i in range(ni // 2):
            total, squares = joined(part[m, half + i, 0], part[m, half + i, 1], got1[m, i, 0], got1[m, i, 1], nj)
            pair[m, i, 0] = total
            pair[m, i, 1] = squares
        sum_copy(1, m).start()

    def stage3(m):
        sum_copy(1, m).wait_recv()
        count = nj * n_rows
        for i in range(ni // 2):
            total, squares = joined(pair[m, i, 0], pair[m, i, 1], got2[m, i, 0], got2[m, i, 1], 2 * nj)
            stats[0, half + i, at(m), :] = total * (1.0 / count)
            stats[1, half + i, at(m), :] = lax.rsqrt(squares * (1.0 / count) + 0.0001)
        sum_copy(2, m).start()

    def stage4(m):
        stats_arrive(m).wait_recv()

    lags = (0, 2, chunks + 2, 2 * chunks + 2)

    def tail(t, x):
        pl.when(t < LATE)(lambda: forward_late(t + (STEPS - 1) * chunks))
        for lag, stage in zip(lags, (stage1, stage2, stage3, stage4)):
            m = t - lag
            pl.when(jnp.logical_and(m >= 0, m < chunks))(lambda m=m, stage=stage: stage(m))
        return x

    lax.fori_loop(0, chunks + lags[-1], tail, 0)

    for way in range(2):
        for n in range(STEPS):
            a = (1, ni)[way]
            whole = u.at[n, pl.ds(1, nj), a, pl.ds(PAD, nk)]
            pl.when(has_col[way])(lambda way=way, n=n, whole=whole: copy_to(whole, whole, col_send.at[way, n], col_recv.at[way, n, 0], {"cols": c + (-1, 1)[way]}).wait_send())
            b = (1, nj)[way]
            face = u.at[n, b, pl.ds(1, ni), pl.ds(PAD, nk)]
            pl.when(has_row[way])(lambda way=way, n=n, face=face: copy_to(face, face, row_send.at[way, n], row_recv.at[way, n, 0], {"rows": r + (-1, 1)[way]}).wait_send())
            pl.when(has_slab[way])(lambda way=way, n=n: slab_copy(way, n).wait_send())
    for n in range(STEPS):
        for way in range(2):
            @pl.when(forwards[way])
            def _(n=n, way=way):
                copy_to(relay.at[n], relay.at[n], relay_send.at[n], relay_recv.at[n, 0], {"rows": r + (-2, 2)[way]}).wait_send()
    for stage, ref in enumerate((got1, pair, got1)):
        copy_to(ref, ref, sum_send.at[stage], sum_recv.at[stage, 0], {"rows": y_partner}).wait_send()


def finish(last, stats, anomaly, field_end, scaled, sems):
    nj, ni, nk, _ = last.shape

    def store(which, i):
        here = (slice(None), pl.ds(i, 1))
        start, end = ((last, field_end), (scaled, anomaly))[which]
        return pltpu.make_async_copy(start.at[here], end.at[here], sems.at[which, i])

    for i in range(ni):
        store(0, i).start()

        def line(q, x):
            at = pl.ds(pl.multiple_of(q * 8, 8), 8)
            mean, scale = stats[0, i, at, :], stats[1, i, at, :]
            for j in range(nj):
                scaled[j, i, at, :] = (last[j, i, at, :] - mean) * scale
            return x

        lax.fori_loop(0, nk // 8, line, 0, unroll=2)
        store(1, i).start()
    for i in range(ni):
        store(0, i).wait()
        store(1, i).wait()


def solution(mesh):
    sizes = (mesh.shape["rows"], mesh.shape["cols"], mesh.shape["slabs"])

    def on_device(field_values, conductance, source):
        shape = field_values.shape
        nj, ni, nk, levels = shape
        chunks = nk // 8
        f32 = jnp.float32
        sem = pltpu.SemaphoreType.DMA
        last, stats = pl.pallas_call(
            functools.partial(kernel, sizes),
            out_shape=(jax.ShapeDtypeStruct(shape, f32), jax.ShapeDtypeStruct((2, ni, nk, levels), f32)),
            in_specs=[pl.BlockSpec(memory_space=pltpu.HBM)] * 3,
            out_specs=(pl.BlockSpec(memory_space=pltpu.VMEM),) * 2,
            scratch_shapes=[
                pltpu.VMEM((STEPS, nj + 2, ni + 2, nk + 2 * PAD, levels), f32),
                pltpu.VMEM(shape, f32),
                pltpu.VMEM(shape, f32),
                pltpu.VMEM((2, STEPS, nj * ni, levels), f32),
                pltpu.VMEM((2, STEPS, nj * ni, levels), f32),
                pltpu.VMEM((STEPS, chunks // 2, ni, 8, levels), f32),
                pltpu.VMEM((chunks, ni, 2, 8, levels), f32),
                pltpu.VMEM((chunks, ni // 2, 2, 8, levels), f32),
                pltpu.VMEM((chunks, ni // 2, 2, 8, levels), f32),
                pltpu.VMEM((chunks, ni // 2, 2, 8, levels), f32),
                sem((STEPS,)),
                sem((STEPS, chunks // 2)),
                sem((3, chunks)),
                sem((2, STEPS)),
                sem((2, STEPS, chunks)),
                sem((2, STEPS)),
                sem((2, STEPS, chunks)),
                sem((2, STEPS)),
                sem((2, STEPS)),
                sem((3,)),
                sem((3, chunks)),
            ],
            compiler_params=pltpu.CompilerParams(
                collective_id=0, has_side_effects=True, vmem_limit_bytes=46 * 2**20
            ),
            name="heat",
        )(field_values, conductance, source)
        return pl.pallas_call(
            finish,
            out_shape=(jax.ShapeDtypeStruct(shape, f32),) * 2,
            in_specs=[pl.BlockSpec(memory_space=pltpu.VMEM)] * 2,
            out_specs=(pl.BlockSpec(memory_space=pltpu.HBM),) * 2,
            scratch_shapes=[pltpu.VMEM(shape, f32), sem((2, ni))],
            compiler_params=pltpu.CompilerParams(vmem_limit_bytes=10 * 2**20),
            name="finish",
        )(last, stats)

    spec = P(("trial", "rows"), "cols", "slabs", None)
    return jax.shard_map(on_device, mesh=mesh, in_specs=(spec,) * 3, out_specs=(spec,) * 2, check_vma=False)
```

```python
import functools

import jax
import jax.numpy as jnp
from jax import lax
from jax.experimental import pallas as pl
from jax.experimental.pallas import tpu as pltpu
from jax.sharding import PartitionSpec as P

STEPS = 4
MESH = pl.DeviceIdType.MESH
WHOLE = 2
LATE = 3
PAD = 8


def copy_to(src, dst, send, recv, device):
    return pltpu.make_async_remote_copy(
        src_ref=src, dst_ref=dst, send_sem=send, recv_sem=recv, device_id=device, device_id_type=MESH
    )


def kernel(
    sizes, field, conductance, source, last, scaled,
    u, cond, src, edge_out, edge_in, relay, part, got1, pair, got2, whole1, whole_pair, whole2, stats,
    relay_send, relay_recv, load_sem, col_send, col_recv, row_send, row_recv, slab_send, slab_recv, sum_send, sum_recv,
):
    n_rows, n_cols, n_slabs = sizes
    nj, ni, nk, _ = field.shape
    chunks = nk // 8
    r, c, s = lax.axis_index("rows"), lax.axis_index("cols"), lax.axis_index("slabs")
    y_partner = r + 1 - 2 * lax.rem(r, 2)
    z_partner = lax.rem(r + 2, 4)
    half = lax.rem(r, 2) * (ni // 2)
    other = (ni // 2) - half

    def chunk_of(m):
        return jnp.where(lax.rem(m, 2) == 0, m // 2, chunks - 1 - m // 2)

    def at(m):
        return pl.ds(pl.multiple_of(chunk_of(m) * 8, 8), 8)

    def padded(m):
        return pl.ds(pl.multiple_of(chunk_of(m) * 8 + PAD, 8), 8)

    def load(which, m):
        here = (slice(None), slice(None), at(m))
        inside = (0, pl.ds(1, nj), pl.ds(1, ni), padded(m))
        pairs = ((field, u, inside), (conductance, cond, here), (source, src, here))
        start, end, place = pairs[which]
        return pltpu.make_async_copy(start.at[here], end.at[place], load_sem.at[which, m])

    def col_copy(way, n, m):
        a, b = ((1, ni + 1), (ni, 0))[way]
        return copy_to(
            u.at[n, pl.ds(1, nj), a, padded(m)], u.at[n, pl.ds(1, nj), b, padded(m)],
            col_send.at[way, n], col_recv.at[way, n, m], {"cols": c + (-1, 1)[way]},
        )

    def row_copy(way, n, m):
        a, b = ((1, nj + 1), (nj, 0))[way]
        return copy_to(
            u.at[n, a, pl.ds(1, ni), padded(m)], u.at[n, b, pl.ds(1, ni), padded(m)],
            row_send.at[way, n], row_recv.at[way, n, m], {"rows": r + (-1, 1)[way]},
        )

    def detour_copy(way, n, m):
        return copy_to(
            u.at[n, (1, nj)[way], pl.ds(1, ni), padded(m)], relay.at[n, m // 2],
            row_send.at[way, n], relay_recv.at[n, m // 2], {"rows": r + (1, -1)[way]},
        )

    def forward_copy(way, n, m):
        return copy_to(
            relay.at[n, m // 2], u.at[n, (nj + 1, 0)[way], pl.ds(1, ni), padded(m)],
            relay_send.at[n], row_recv.at[way, n, m], {"rows": r + (-2, 2)[way]},
        )

    crosses = (r == 2, r == 1)
    forwards = (r == 3, r == 0)

    def forward(n, m):
        for way in range(2):
            @pl.when(jnp.logical_and(forwards[way], lax.rem(m, 2) == 1))
            def _(way=way):
                detour_copy(way, n, m).wait_recv()
                forward_copy(way, n, m).start()

    def slab_copy(way, n):
        return copy_to(
            edge_out.at[way, n], edge_in.at[way, n],
            slab_send.at[way, n], slab_recv.at[way, n], {"slabs": s + (-1, 1)[way]},
        )

    has_col = (c > 0, c < n_cols - 1)
    has_row = (r > 0, r < n_rows - 1)
    has_slab = (s > 0, s < n_slabs - 1)

    def send_faces(n, m):
        for way in range(2):
            detour = jnp.logical_and(crosses[way], lax.rem(m, 2) == 1)
            pl.when(detour)(lambda way=way: detour_copy(way, n, m).start())
            pl.when(jnp.logical_and(has_row[way], jnp.logical_not(detour)))(lambda way=way: row_copy(way, n, m).start())
        for way in range(2):
            pl.when(has_col[way])(lambda way=way: col_copy(way, n, m).start())
        for way in range(2):
            @pl.when(jnp.logical_and(has_slab[way], m == way))
            def _(way=way):
                k = (PAD, PAD + nk - 1)[way]
                for j in range(nj):
                    for i in range(ni):
                        edge_out[way, n, pl.ds(j * ni + i, 1), :] = u[n, j + 1, i + 1, pl.ds(k, 1), :]
                slab_copy(way, n).start()

    def take_faces(n, m):
        for way in range(2):
            pl.when(has_col[1 - way])(lambda way=way: col_copy(way, n, m).wait_recv())
            pl.when(has_row[1 - way])(lambda way=way: row_copy(way, n, m).wait_recv())
        for way in range(2):
            @pl.when(jnp.logical_and(has_slab[1 - way], m == 1 - way))
            def _(way=way):
                slab_copy(way, n).wait_recv()
                k = (PAD + nk, PAD - 1)[way]
                for j in range(nj):
                    for i in range(ni):
                        u[n, j + 1, i + 1, pl.ds(k, 1), :] = edge_in[way, n, pl.ds(j * ni + i, 1), :]

    def sum_copy(stage, m):
        if stage == 0:
            return copy_to(part.at[m, pl.ds(other, ni // 2)], got1.at[m], sum_send.at[0], sum_recv.at[0, m], {"rows": y_partner})
        if stage == 1:
            return copy_to(pair.at[m], got2.at[m], sum_send.at[1], sum_recv.at[1, m], {"rows": z_partner})
        mine = stats.at[:, pl.ds(half, ni // 2), at(m)]
        return copy_to(mine, mine, sum_send.at[2], sum_recv.at[2, m], {"rows": y_partner})

    def whole_copy(stage, m):
        k = m - (chunks - WHOLE)
        start, end, peer = ((part.at[m], whole1.at[k], y_partner), (whole_pair.at[k], whole2.at[k], z_partner))[stage]
        return copy_to(start, end, sum_send.at[3 + stage], sum_recv.at[stage, m], {"rows": peer})

    def stats_arrive(m):
        theirs = stats.at[:, pl.ds(other, ni // 2), at(m)]
        return copy_to(theirs, theirs, sum_send.at[2], sum_recv.at[2, m], {"rows": y_partner})

    def updated(n, j, i, m, below):
        k0 = chunk_of(m) * 8 + PAD
        middle = u[n, j + 1, i + 1, padded(m), :]
        above = u[n, j + 2, i + 1, padded(m), :]
        spread = below + above + u[n, j + 1, i, padded(m), :] + u[n, j + 1, i + 2, padded(m), :]
        spread = spread + u[n, j + 1, i + 1, pl.ds(k0 - 1, 8), :] + u[n, j + 1, i + 1, pl.ds(k0 + 1, 8), :]
        spread = spread - 6.0 * middle
        return middle, middle + cond[j, i, at(m), :] * spread + src[j, i, at(m), :]

    def step_chunk(n, m):
        def row(j, below):
            out = []
            for i in range(ni):
                middle, new = updated(n, j, i, m, below[i])
                u[n + 1, j + 1, i + 1, padded(m), :] = new
                out.append(middle)
            return tuple(out)

        lax.fori_loop(0, nj, row, tuple(u[n, 0, i + 1, padded(m), :] for i in range(ni)), unroll=2)

    def last_chunk(m):
        n = STEPS - 1

        def row(j, carry):
            below, total = carry
            out, sums = [], []
            for i in range(ni):
                middle, new = updated(n, j, i, m, below[i])
                last[j, i, at(m), :] = new
                out.append(middle)
                sums.append(total[i] + new)
            return tuple(out), tuple(sums)

        zero = jnp.zeros((8, 128), jnp.float32)
        start = tuple(u[n, 0, i + 1, padded(m), :] for i in range(ni))
        _, total = lax.fori_loop(0, nj, row, (start, (zero,) * ni), unroll=2)

        def spread_row(j, squares):
            out = []
            for i in range(ni):
                d = last[j, i, at(m), :] - total[i] * (1.0 / nj)
                out.append(squares[i] + d * d)
            return tuple(out)

        squares = lax.fori_loop(0, nj, spread_row, (zero,) * ni, unroll=4)
        for i in range(ni):
            part[m, i, 0] = total[i]
            part[m, i, 1] = squares[i]

    def joined(a_sum, a_sq, b_sum, b_sq, count):
        d = a_sum - b_sum
        return a_sum + b_sum, a_sq + b_sq + d * d * (0.5 / count)

    barrier = pltpu.get_barrier_semaphore()
    for way in range(2):
        step = (-1, 1)[way]
        pl.when(has_col[way])(lambda step=step: pl.semaphore_signal(barrier, inc=1, device_id={"cols": c + step}, device_id_type=MESH))
        pl.when(has_slab[way])(lambda step=step: pl.semaphore_signal(barrier, inc=1, device_id={"slabs": s + step}, device_id_type=MESH))
    for d in range(1, n_rows):
        pl.semaphore_signal(barrier, inc=1, device_id={"rows": lax.rem(r + d, n_rows)}, device_id_type=MESH)
    for m in range(chunks):
        load(0, m).start()
    for m in range(chunks):
        load(1, m).start()
        load(2, m).start()

    zero = jnp.zeros((8, 128), jnp.float32)

    def clear_cols(i):
        def body(q, x):
            n, j = q // nj, lax.rem(q, nj)
            for k in range(chunks):
                u[n, j + 1, i, pl.ds(PAD + 8 * k, 8), :] = zero
            return x
        lax.fori_loop(0, STEPS * nj, body, 0)

    def clear_rows(j):
        def body(q, x):
            n, i = q // ni, lax.rem(q, ni)
            for k in range(chunks):
                u[n, j, i + 1, pl.ds(PAD + 8 * k, 8), :] = zero
            return x
        lax.fori_loop(0, STEPS * ni, body, 0)

    def clear_slabs(k):
        def body(q, x):
            n, j = q // nj, lax.rem(q, nj)
            for i in range(ni):
                u[n, j + 1, i + 1, pl.ds(k, 8), :] = zero
            return x
        lax.fori_loop(0, STEPS * nj, body, 0)

    pl.when(c == 0)(lambda: clear_cols(0))
    pl.when(c == n_cols - 1)(lambda: clear_cols(ni + 1))
    pl.when(r == 0)(lambda: clear_rows(0))
    pl.when(r == n_rows - 1)(lambda: clear_rows(nj + 1))
    pl.when(s == 0)(lambda: clear_slabs(0))
    pl.when(s == n_slabs - 1)(lambda: clear_slabs(PAD + nk))

    one = lambda flag: jnp.where(flag, 1, 0)
    pl.semaphore_wait(barrier, n_rows - 1 + one(has_col[0]) + one(has_col[1]) + one(has_slab[0]) + one(has_slab[1]))

    def first(m, x):
        load(0, m).wait()
        send_faces(0, m)
        forward(0, m)
        return x

    lax.fori_loop(0, chunks, first, 0)

    def forward_late(q):
        p = q - LATE
        pl.when(p >= 0)(lambda: forward(p // chunks + 1, lax.rem(p, chunks)))

    def steps(q, x):
        n, m = q // chunks, lax.rem(q, chunks)
        forward_late(q)

        @pl.when(n == 0)
        def _():
            load(1, m).wait()
            load(2, m).wait()

        take_faces(n, m)
        step_chunk(n, m)
        pl.when(q > 0)(lambda: send_faces((q - 1) // chunks + 1, lax.rem(q - 1, chunks)))
        return x

    lax.fori_loop(0, (STEPS - 1) * chunks, steps, 0)

    send_faces(STEPS - 1, chunks - 1)

    def stage1(m):
        take_faces(STEPS - 1, m)
        last_chunk(m)
        pl.when(m < chunks - WHOLE)(lambda: sum_copy(0, m).start())
        pl.when(m >= chunks - WHOLE)(lambda: whole_copy(0, m).start())

    def stage2(m):
        sum_copy(0, m).wait_recv()
        for i in range(ni // 2):
            total, squares = joined(part[m, half + i, 0], part[m, half + i, 1], got1[m, i, 0], got1[m, i, 1], nj)
            pair[m, i, 0] = total
            pair[m, i, 1] = squares
        sum_copy(1, m).start()

    def stage3(m):
        sum_copy(1, m).wait_recv()
        count = nj * n_rows
        for i in range(ni // 2):
            total, squares = joined(pair[m, i, 0], pair[m, i, 1], got2[m, i, 0], got2[m, i, 1], 2 * nj)
            stats[0, half + i, at(m), :] = total * (1.0 / count)
            stats[1, half + i, at(m), :] = lax.rsqrt(squares * (1.0 / count) + 0.0001)
        sum_copy(2, m).start()

    def scale_chunk(m):
        mean = [stats[0, i, at(m), :] for i in range(ni)]
        scale = [stats[1, i, at(m), :] for i in range(ni)]

        def row(j, x):
            for i in range(ni):
                scaled[j, i, at(m), :] = (last[j, i, at(m), :] - mean[i]) * scale[i]
            return x

        lax.fori_loop(0, nj, row, 0, unroll=4)

    def stage4(m):
        stats_arrive(m).wait_recv()
        scale_chunk(m)

    def whole_stage2(m):
        k = m - (chunks - WHOLE)
        whole_copy(0, m).wait_recv()
        for i in range(ni):
            total, squares = joined(part[m, i, 0], part[m, i, 1], whole1[k, i, 0], whole1[k, i, 1], nj)
            whole_pair[k, i, 0] = total
            whole_pair[k, i, 1] = squares
        whole_copy(1, m).start()

    def whole_stage3(m):
        k = m - (chunks - WHOLE)
        whole_copy(1, m).wait_recv()
        count = nj * n_rows
        for i in range(ni):
            total, squares = joined(whole_pair[k, i, 0], whole_pair[k, i, 1], whole2[k, i, 0], whole2[k, i, 1], 2 * nj)
            stats[0, i, at(m), :] = total * (1.0 / count)
            stats[1, i, at(m), :] = lax.rsqrt(squares * (1.0 / count) + 0.0001)
        scale_chunk(m)

    lags = (0, 2, chunks + 2, chunks + 8)

    def tail(t, x):
        pl.when(t < LATE)(lambda: forward_late(t + (STEPS - 1) * chunks))
        split = chunks - WHOLE
        for lag, stage, rest in zip(lags, (stage1, stage2, stage3, stage4), (stage1, whole_stage2, whole_stage3, None)):
            m = t - lag
            if stage is rest:
                pl.when(m < chunks)(lambda m=m: stage1(m))
                continue
            pl.when(jnp.logical_and(m >= 0, m < split))(lambda m=m, stage=stage: stage(m))
            if rest is not None:
                pl.when(jnp.logical_and(m >= split, m < chunks))(lambda m=m, rest=rest: rest(m))
        return x

    lax.fori_loop(0, chunks - WHOLE + lags[-1], tail, 0)

    for way in range(2):
        for n in range(STEPS):
            a = (1, ni)[way]
            whole = u.at[n, pl.ds(1, nj), a, pl.ds(PAD, nk)]
            pl.when(has_col[way])(lambda way=way, n=n, whole=whole: copy_to(whole, whole, col_send.at[way, n], col_recv.at[way, n, 0], {"cols": c + (-1, 1)[way]}).wait_send())
            b = (1, nj)[way]
            face = u.at[n, b, pl.ds(1, ni), pl.ds(PAD, nk)]
            pl.when(has_row[way])(lambda way=way, n=n, face=face: copy_to(face, face, row_send.at[way, n], row_recv.at[way, n, 0], {"rows": r + (-1, 1)[way]}).wait_send())
            pl.when(has_slab[way])(lambda way=way, n=n: slab_copy(way, n).wait_send())
    for n in range(STEPS):
        for way in range(2):
            @pl.when(forwards[way])
            def _(n=n, way=way):
                copy_to(relay.at[n], relay.at[n], relay_send.at[n], relay_recv.at[n, 0], {"rows": r + (-2, 2)[way]}).wait_send()
    most = pl.ds(0, chunks - WHOLE)
    for stage, ref in enumerate((got1.at[most], pair.at[most], got1.at[most], whole1, whole_pair)):
        copy_to(ref, ref, sum_send.at[stage], sum_recv.at[0, 0], {"rows": y_partner}).wait_send()


def finish(last, scaled, anomaly, field_end, sems):
    parts = sems.shape[1]
    rows = last.shape[0] // parts

    def store(which, b):
        here = pl.ds(b * rows, rows)
        start, end = ((last, field_end), (scaled, anomaly))[which]
        return pltpu.make_async_copy(start.at[here], end.at[here], sems.at[which, b])

    for b in range(parts):
        store(0, b).start()
        store(1, b).start()
    for b in range(parts):
        store(0, b).wait()
        store(1, b).wait()


def solution(mesh):
    sizes = (mesh.shape["rows"], mesh.shape["cols"], mesh.shape["slabs"])

    def on_device(field_values, conductance, source):
        shape = field_values.shape
        nj, ni, nk, levels = shape
        chunks = nk // 8
        f32 = jnp.float32
        sem = pltpu.SemaphoreType.DMA
        last, scaled = pl.pallas_call(
            functools.partial(kernel, sizes),
            out_shape=(jax.ShapeDtypeStruct(shape, f32),) * 2,
            in_specs=[pl.BlockSpec(memory_space=pltpu.HBM)] * 3,
            out_specs=(pl.BlockSpec(memory_space=pltpu.VMEM),) * 2,
            scratch_shapes=[
                pltpu.VMEM((STEPS, nj + 2, ni + 2, nk + 2 * PAD, levels), f32),
                pltpu.VMEM(shape, f32),
                pltpu.VMEM(shape, f32),
                pltpu.VMEM((2, STEPS, nj * ni, levels), f32),
                pltpu.VMEM((2, STEPS, nj * ni, levels), f32),
                pltpu.VMEM((STEPS, chunks // 2, ni, 8, levels), f32),
                pltpu.VMEM((chunks, ni, 2, 8, levels), f32),
                pltpu.VMEM((chunks, ni // 2, 2, 8, levels), f32),
                pltpu.VMEM((chunks, ni // 2, 2, 8, levels), f32),
                pltpu.VMEM((chunks, ni // 2, 2, 8, levels), f32),
                pltpu.VMEM((WHOLE, ni, 2, 8, levels), f32),
                pltpu.VMEM((WHOLE, ni, 2, 8, levels), f32),
                pltpu.VMEM((WHOLE, ni, 2, 8, levels), f32),
                pltpu.VMEM((2, ni, nk, levels), f32),
                sem((STEPS,)),
                sem((STEPS, chunks // 2)),
                sem((3, chunks)),
                sem((2, STEPS)),
                sem((2, STEPS, chunks)),
                sem((2, STEPS)),
                sem((2, STEPS, chunks)),
                sem((2, STEPS)),
                sem((2, STEPS)),
                sem((5,)),
                sem((3, chunks)),
            ],
            compiler_params=pltpu.CompilerParams(
                collective_id=0, has_side_effects=True, vmem_limit_bytes=43 * 2**20
            ),
            name="heat",
        )(field_values, conductance, source)
        return pl.pallas_call(
            finish,
            out_shape=(jax.ShapeDtypeStruct(shape, f32),) * 2,
            in_specs=[pl.BlockSpec(memory_space=pltpu.VMEM)] * 2,
            out_specs=(pl.BlockSpec(memory_space=pltpu.HBM),) * 2,
            scratch_shapes=[sem((2, 4))],
            compiler_params=pltpu.CompilerParams(vmem_limit_bytes=4 * 2**20),
            name="finish",
        )(last, scaled)

    spec = P(("trial", "rows"), "cols", "slabs", None)
    return jax.shard_map(on_device, mesh=mesh, in_specs=(spec,) * 3, out_specs=(spec,) * 2, check_vma=False)
```

```python
import functools

import jax
import jax.numpy as jnp
from jax import lax
from jax.experimental import pallas as pl
from jax.experimental.pallas import tpu as pltpu
from jax.sharding import PartitionSpec as P

STEPS = 4
MESH = pl.DeviceIdType.MESH
WHOLE = 2
LATE = 3
PAD = 8


def copy_to(src, dst, send, recv, device):
    return pltpu.make_async_remote_copy(
        src_ref=src, dst_ref=dst, send_sem=send, recv_sem=recv, device_id=device, device_id_type=MESH
    )


def kernel(
    sizes, field, conductance, source, last, scaled,
    u, cond, src, edge_out, edge_in, relay, part, got1, pair, got2, whole1, whole_pair, whole2, stats,
    relay_send, relay_recv, load_sem, col_send, col_recv, row_send, row_recv, slab_send, slab_recv, sum_send, sum_recv,
):
    n_rows, n_cols, n_slabs = sizes
    nj, ni, nk, _ = field.shape
    chunks = nk // 8
    r, c, s = lax.axis_index("rows"), lax.axis_index("cols"), lax.axis_index("slabs")
    y_partner = r + 1 - 2 * lax.rem(r, 2)
    z_partner = lax.rem(r + 2, 4)
    half = lax.rem(r, 2) * (ni // 2)
    other = (ni // 2) - half

    def chunk_of(m):
        return jnp.where(lax.rem(m, 2) == 0, m // 2, chunks - 1 - m // 2)

    def at(m):
        return pl.ds(pl.multiple_of(chunk_of(m) * 8, 8), 8)

    def padded(m):
        return pl.ds(pl.multiple_of(chunk_of(m) * 8 + PAD, 8), 8)

    def load(which, m):
        here = (slice(None), slice(None), at(m))
        inside = (0, pl.ds(1, nj), pl.ds(1, ni), padded(m))
        pairs = ((field, u, inside), (conductance, cond, here), (source, src, here))
        start, end, place = pairs[which]
        return pltpu.make_async_copy(start.at[here], end.at[place], load_sem.at[which, m])

    def col_copy(way, n, m):
        a, b = ((1, ni + 1), (ni, 0))[way]
        return copy_to(
            u.at[n, pl.ds(1, nj), a, padded(m)], u.at[n, pl.ds(1, nj), b, padded(m)],
            col_send.at[way, n], col_recv.at[way, n, m], {"cols": c + (-1, 1)[way]},
        )

    def row_copy(way, n, m):
        a, b = ((1, nj + 1), (nj, 0))[way]
        return copy_to(
            u.at[n, a, pl.ds(1, ni), padded(m)], u.at[n, b, pl.ds(1, ni), padded(m)],
            row_send.at[way, n], row_recv.at[way, n, m], {"rows": r + (-1, 1)[way]},
        )

    def detour_copy(way, n, m):
        return copy_to(
            u.at[n, (1, nj)[way], pl.ds(1, ni), padded(m)], relay.at[n, m // 2],
            row_send.at[way, n], relay_recv.at[n, m // 2], {"rows": r + (1, -1)[way]},
        )

    def forward_copy(way, n, m):
        return copy_to(
            relay.at[n, m // 2], u.at[n, (nj + 1, 0)[way], pl.ds(1, ni), padded(m)],
            relay_send.at[n], row_recv.at[way, n, m], {"rows": r + (-2, 2)[way]},
        )

    crosses = (r == 2, r == 1)
    forwards = (r == 3, r == 0)

    def forward(n, m):
        for way in range(2):
            @pl.when(jnp.logical_and(forwards[way], lax.rem(m, 2) == 1))
            def _(way=way):
                detour_copy(way, n, m).wait_recv()
                forward_copy(way, n, m).start()

    def slab_copy(way, n):
        return copy_to(
            edge_out.at[way, n], edge_in.at[way, n],
            slab_send.at[way, n], slab_recv.at[way, n], {"slabs": s + (-1, 1)[way]},
        )

    has_col = (c > 0, c < n_cols - 1)
    has_row = (r > 0, r < n_rows - 1)
    has_slab = (s > 0, s < n_slabs - 1)

    def send_faces(n, m):
        for way in range(2):
            detour = jnp.logical_and(crosses[way], lax.rem(m, 2) == 1)
            pl.when(detour)(lambda way=way: detour_copy(way, n, m).start())
            pl.when(jnp.logical_and(has_row[way], jnp.logical_not(detour)))(lambda way=way: row_copy(way, n, m).start())
        for way in range(2):
            pl.when(has_col[way])(lambda way=way: col_copy(way, n, m).start())
        for way in range(2):
            @pl.when(jnp.logical_and(has_slab[way], m == way))
            def _(way=way):
                k = (PAD, PAD + nk - 1)[way]
                for j in range(nj):
                    for i in range(ni):
                        edge_out[way, n, pl.ds(j * ni + i, 1), :] = u[n, j + 1, i + 1, pl.ds(k, 1), :]
                slab_copy(way, n).start()

    def take_faces(n, m):
        for way in range(2):
            pl.when(has_col[1 - way])(lambda way=way: col_copy(way, n, m).wait_recv())
            pl.when(has_row[1 - way])(lambda way=way: row_copy(way, n, m).wait_recv())
        for way in range(2):
            @pl.when(jnp.logical_and(has_slab[1 - way], m == 1 - way))
            def _(way=way):
                slab_copy(way, n).wait_recv()
                k = (PAD + nk, PAD - 1)[way]
                for j in range(nj):
                    for i in range(ni):
                        u[n, j + 1, i + 1, pl.ds(k, 1), :] = edge_in[way, n, pl.ds(j * ni + i, 1), :]

    def sum_copy(stage, m):
        if stage == 0:
            return copy_to(part.at[m, pl.ds(other, ni // 2)], got1.at[m], sum_send.at[0], sum_recv.at[0, m], {"rows": y_partner})
        if stage == 1:
            return copy_to(pair.at[m], got2.at[m], sum_send.at[1], sum_recv.at[1, m], {"rows": z_partner})
        mine = stats.at[:, pl.ds(half, ni // 2), at(m)]
        return copy_to(mine, mine, sum_send.at[2], sum_recv.at[2, m], {"rows": y_partner})

    def whole_copy(stage, m):
        k = m - (chunks - WHOLE)
        start, end, peer = ((part.at[m], whole1.at[k], y_partner), (whole_pair.at[k], whole2.at[k], z_partner))[stage]
        return copy_to(start, end, sum_send.at[3 + stage], sum_recv.at[stage, m], {"rows": peer})

    def stats_arrive(m):
        theirs = stats.at[:, pl.ds(other, ni // 2), at(m)]
        return copy_to(theirs, theirs, sum_send.at[2], sum_recv.at[2, m], {"rows": y_partner})

    def updated(n, j, i, m, below):
        k0 = chunk_of(m) * 8 + PAD
        middle = u[n, j + 1, i + 1, padded(m), :]
        above = u[n, j + 2, i + 1, padded(m), :]
        spread = below + above + u[n, j + 1, i, padded(m), :] + u[n, j + 1, i + 2, padded(m), :]
        spread = spread + u[n, j + 1, i + 1, pl.ds(k0 - 1, 8), :] + u[n, j + 1, i + 1, pl.ds(k0 + 1, 8), :]
        spread = spread - 6.0 * middle
        return middle, middle + cond[j, i, at(m), :] * spread + src[j, i, at(m), :]

    def step_chunk(n, m):
        def row(j, below):
            out = []
            for i in range(ni):
                middle, new = updated(n, j, i, m, below[i])
                u[n + 1, j + 1, i + 1, padded(m), :] = new
                out.append(middle)
            return tuple(out)

        lax.fori_loop(0, nj, row, tuple(u[n, 0, i + 1, padded(m), :] for i in range(ni)), unroll=2)

    def last_chunk(m):
        n = STEPS - 1

        def row(j, carry):
            below, total = carry
            out, sums = [], []
            for i in range(ni):
                middle, new = updated(n, j, i, m, below[i])
                last[j, i, at(m), :] = new
                out.append(middle)
                sums.append(total[i] + new)
            return tuple(out), tuple(sums)

        zero = jnp.zeros((8, 128), jnp.float32)
        start = tuple(u[n, 0, i + 1, padded(m), :] for i in range(ni))
        _, total = lax.fori_loop(0, nj, row, (start, (zero,) * ni), unroll=2)

        def spread_row(j, squares):
            out = []
            for i in range(ni):
                d = last[j, i, at(m), :] - total[i] * (1.0 / nj)
                out.append(squares[i] + d * d)
            return tuple(out)

        squares = lax.fori_loop(0, nj, spread_row, (zero,) * ni, unroll=4)
        for i in range(ni):
            part[m, i, 0] = total[i]
            part[m, i, 1] = squares[i]

    def joined(a_sum, a_sq, b_sum, b_sq, count):
        d = a_sum - b_sum
        return a_sum + b_sum, a_sq + b_sq + d * d * (0.5 / count)

    barrier = pltpu.get_barrier_semaphore()
    for way in range(2):
        step = (-1, 1)[way]
        pl.when(has_col[way])(lambda step=step: pl.semaphore_signal(barrier, inc=1, device_id={"cols": c + step}, device_id_type=MESH))
        pl.when(has_slab[way])(lambda step=step: pl.semaphore_signal(barrier, inc=1, device_id={"slabs": s + step}, device_id_type=MESH))
    for d in range(1, n_rows):
        pl.semaphore_signal(barrier, inc=1, device_id={"rows": lax.rem(r + d, n_rows)}, device_id_type=MESH)
    for m in range(chunks):
        load(0, m).start()
    for m in range(chunks):
        load(1, m).start()
        load(2, m).start()

    zero = jnp.zeros((8, 128), jnp.float32)

    def clear_cols(i):
        def body(q, x):
            n, j = q // nj, lax.rem(q, nj)
            for k in range(chunks):
                u[n, j + 1, i, pl.ds(PAD + 8 * k, 8), :] = zero
            return x
        lax.fori_loop(0, STEPS * nj, body, 0)

    def clear_rows(j):
        def body(q, x):
            n, i = q // ni, lax.rem(q, ni)
            for k in range(chunks):
                u[n, j, i + 1, pl.ds(PAD + 8 * k, 8), :] = zero
            return x
        lax.fori_loop(0, STEPS * ni, body, 0)

    def clear_slabs(k):
        def body(q, x):
            n, j = q // nj, lax.rem(q, nj)
            for i in range(ni):
                u[n, j + 1, i + 1, pl.ds(k, 8), :] = zero
            return x
        lax.fori_loop(0, STEPS * nj, body, 0)

    pl.when(c == 0)(lambda: clear_cols(0))
    pl.when(c == n_cols - 1)(lambda: clear_cols(ni + 1))
    pl.when(r == 0)(lambda: clear_rows(0))
    pl.when(r == n_rows - 1)(lambda: clear_rows(nj + 1))
    pl.when(s == 0)(lambda: clear_slabs(0))
    pl.when(s == n_slabs - 1)(lambda: clear_slabs(PAD + nk))

    one = lambda flag: jnp.where(flag, 1, 0)
    pl.semaphore_wait(barrier, n_rows - 1 + one(has_col[0]) + one(has_col[1]) + one(has_slab[0]) + one(has_slab[1]))

    def first(m, x):
        load(0, m).wait()
        send_faces(0, m)
        forward(0, m)
        return x

    lax.fori_loop(0, chunks, first, 0)

    def forward_late(q):
        p = q - LATE
        pl.when(p >= 0)(lambda: forward(p // chunks + 1, lax.rem(p, chunks)))

    def steps(q, x):
        n, m = q // chunks, lax.rem(q, chunks)
        forward_late(q)

        @pl.when(n == 0)
        def _():
            load(1, m).wait()
            load(2, m).wait()

        take_faces(n, m)
        step_chunk(n, m)
        pl.when(q > 0)(lambda: send_faces((q - 1) // chunks + 1, lax.rem(q - 1, chunks)))
        return x

    lax.fori_loop(0, (STEPS - 1) * chunks, steps, 0)

    send_faces(STEPS - 1, chunks - 1)

    def stage1(m):
        take_faces(STEPS - 1, m)
        last_chunk(m)
        pl.when(m < chunks - WHOLE)(lambda: sum_copy(0, m).start())
        pl.when(m >= chunks - WHOLE)(lambda: whole_copy(0, m).start())

    def stage2(m):
        sum_copy(0, m).wait_recv()
        for i in range(ni // 2):
            total, squares = joined(part[m, half + i, 0], part[m, half + i, 1], got1[m, i, 0], got1[m, i, 1], nj)
            pair[m, i, 0] = total
            pair[m, i, 1] = squares
        sum_copy(1, m).start()

    def stage3(m):
        sum_copy(1, m).wait_recv()
        count = nj * n_rows
        for i in range(ni // 2):
            total, squares = joined(pair[m, i, 0], pair[m, i, 1], got2[m, i, 0], got2[m, i, 1], 2 * nj)
            stats[0, half + i, at(m), :] = total * (1.0 / count)
            stats[1, half + i, at(m), :] = lax.rsqrt(squares * (1.0 / count) + 0.0001)
        sum_copy(2, m).start()

    def scale_chunk(m):
        mean = [stats[0, i, at(m), :] for i in range(ni)]
        scale = [stats[1, i, at(m), :] for i in range(ni)]

        def row(j, x):
            for i in range(ni):
                scaled[j, i, at(m), :] = (last[j, i, at(m), :] - mean[i]) * scale[i]
            return x

        lax.fori_loop(0, nj, row, 0, unroll=4)

    def stage4(m):
        stats_arrive(m).wait_recv()
        scale_chunk(m)

    def whole_stage2(m):
        k = m - (chunks - WHOLE)
        whole_copy(0, m).wait_recv()
        for i in range(ni):
            total, squares = joined(part[m, i, 0], part[m, i, 1], whole1[k, i, 0], whole1[k, i, 1], nj)
            whole_pair[k, i, 0] = total
            whole_pair[k, i, 1] = squares
        whole_copy(1, m).start()

    def whole_stage3(m):
        k = m - (chunks - WHOLE)
        whole_copy(1, m).wait_recv()
        count = nj * n_rows
        for i in range(ni):
            total, squares = joined(whole_pair[k, i, 0], whole_pair[k, i, 1], whole2[k, i, 0], whole2[k, i, 1], 2 * nj)
            stats[0, i, at(m), :] = total * (1.0 / count)
            stats[1, i, at(m), :] = lax.rsqrt(squares * (1.0 / count) + 0.0001)
        scale_chunk(m)

    lags = (0, 2, chunks + 2, chunks + 8)

    def tail(t, x):
        pl.when(t < LATE)(lambda: forward_late(t + (STEPS - 1) * chunks))
        split = chunks - WHOLE
        for lag, stage, rest in zip(lags, (stage1, stage2, stage3, stage4), (stage1, whole_stage2, whole_stage3, None)):
            m = t - lag
            if stage is rest:
                pl.when(m < chunks)(lambda m=m: stage1(m))
                continue
            pl.when(jnp.logical_and(m >= 0, m < split))(lambda m=m, stage=stage: stage(m))
            if rest is not None:
                pl.when(jnp.logical_and(m >= split, m < chunks))(lambda m=m, rest=rest: rest(m))
        return x

    lax.fori_loop(0, chunks - WHOLE + lags[-1], tail, 0)

    for way in range(2):
        for n in range(STEPS):
            a = (1, ni)[way]
            whole = u.at[n, pl.ds(1, nj), a, pl.ds(PAD, nk)]
            pl.when(has_col[way])(lambda way=way, n=n, whole=whole: copy_to(whole, whole, col_send.at[way, n], col_recv.at[way, n, 0], {"cols": c + (-1, 1)[way]}).wait_send())
            b = (1, nj)[way]
            face = u.at[n, b, pl.ds(1, ni), pl.ds(PAD, nk)]
            pl.when(has_row[way])(lambda way=way, n=n, face=face: copy_to(face, face, row_send.at[way, n], row_recv.at[way, n, 0], {"rows": r + (-1, 1)[way]}).wait_send())
            pl.when(has_slab[way])(lambda way=way, n=n: slab_copy(way, n).wait_send())
    for n in range(STEPS):
        for way in range(2):
            @pl.when(forwards[way])
            def _(n=n, way=way):
                copy_to(relay.at[n], relay.at[n], relay_send.at[n], relay_recv.at[n, 0], {"rows": r + (-2, 2)[way]}).wait_send()
    most = pl.ds(0, chunks - WHOLE)
    for stage, ref in enumerate((got1.at[most], pair.at[most], got1.at[most], whole1, whole_pair)):
        copy_to(ref, ref, sum_send.at[stage], sum_recv.at[0, 0], {"rows": y_partner}).wait_send()


def finish(last, scaled, anomaly, field_end, sems):
    parts = sems.shape[1]
    rows = last.shape[0] // parts

    def store(which, b):
        here = pl.ds(b * rows, rows)
        start, end = ((last, field_end), (scaled, anomaly))[which]
        return pltpu.make_async_copy(start.at[here], end.at[here], sems.at[which, b])

    for b in range(parts):
        store(0, b).start(priority=0)
        store(1, b).start(priority=1)
    for b in range(parts):
        store(0, b).wait()
        store(1, b).wait()


def solution(mesh):
    sizes = (mesh.shape["rows"], mesh.shape["cols"], mesh.shape["slabs"])

    def on_device(field_values, conductance, source):
        shape = field_values.shape
        nj, ni, nk, levels = shape
        chunks = nk // 8
        f32 = jnp.float32
        sem = pltpu.SemaphoreType.DMA
        last, scaled = pl.pallas_call(
            functools.partial(kernel, sizes),
            out_shape=(jax.ShapeDtypeStruct(shape, f32),) * 2,
            in_specs=[pl.BlockSpec(memory_space=pltpu.HBM)] * 3,
            out_specs=(pl.BlockSpec(memory_space=pltpu.VMEM),) * 2,
            scratch_shapes=[
                pltpu.VMEM((STEPS, nj + 2, ni + 2, nk + 2 * PAD, levels), f32),
                pltpu.VMEM(shape, f32),
                pltpu.VMEM(shape, f32),
                pltpu.VMEM((2, STEPS, nj * ni, levels), f32),
                pltpu.VMEM((2, STEPS, nj * ni, levels), f32),
                pltpu.VMEM((STEPS, chunks // 2, ni, 8, levels), f32),
                pltpu.VMEM((chunks, ni, 2, 8, levels), f32),
                pltpu.VMEM((chunks, ni // 2, 2, 8, levels), f32),
                pltpu.VMEM((chunks, ni // 2, 2, 8, levels), f32),
                pltpu.VMEM((chunks, ni // 2, 2, 8, levels), f32),
                pltpu.VMEM((WHOLE, ni, 2, 8, levels), f32),
                pltpu.VMEM((WHOLE, ni, 2, 8, levels), f32),
                pltpu.VMEM((WHOLE, ni, 2, 8, levels), f32),
                pltpu.VMEM((2, ni, nk, levels), f32),
                sem((STEPS,)),
                sem((STEPS, chunks // 2)),
                sem((3, chunks)),
                sem((2, STEPS)),
                sem((2, STEPS, chunks)),
                sem((2, STEPS)),
                sem((2, STEPS, chunks)),
                sem((2, STEPS)),
                sem((2, STEPS)),
                sem((5,)),
                sem((3, chunks)),
            ],
            compiler_params=pltpu.CompilerParams(
                collective_id=0, has_side_effects=True, vmem_limit_bytes=43 * 2**20
            ),
            name="heat",
        )(field_values, conductance, source)
        return pl.pallas_call(
            finish,
            out_shape=(jax.ShapeDtypeStruct(shape, f32),) * 2,
            in_specs=[pl.BlockSpec(memory_space=pltpu.VMEM)] * 2,
            out_specs=(pl.BlockSpec(memory_space=pltpu.HBM),) * 2,
            scratch_shapes=[sem((2, 4))],
            compiler_params=pltpu.CompilerParams(vmem_limit_bytes=4 * 2**20),
            name="finish",
        )(last, scaled)

    spec = P(("trial", "rows"), "cols", "slabs", None)
    return jax.shard_map(on_device, mesh=mesh, in_specs=(spec,) * 3, out_specs=(spec,) * 2, check_vma=False)
```
